32 devices in a mesh: dp: 1 (over z), sp: 32 (over x, y, core).
Axes of the slice: x: 4, y: 4, z: 1, core: 2. Of those that a mesh axis runs over, the one named last changes fastest.
The devices are a block of a 4x4x8 slice.
Arguments:
- q: bfloat16 [32, 20, 128], P('dp')
- k: bfloat16 [32, 8192, 20, 128], P('dp', 'sp')
- v: bfloat16 [32, 8192, 20, 128], P('dp', 'sp')
Outputs:
- q: bfloat16 [32, 20, 128], P('dp')
All inputs are finite; a program needn't handle non-finite values.
Results may differ from the reference program's by a relative error of at most 0.012.
Values are sent between devices in bfloat16 or wider.
A program may use at most 768 MiB of HBM per device.

```python
import jax
import jax.numpy as jnp

BATCH = 32
CACHE = 8192
HEADS = 20
KV_HEADS = 20
HEAD = 128


def setup_inputs(seed: int = 0, part: int = 0) -> dict:
    kq, kk, kv = (jax.random.fold_in(k, part) for k in jax.random.split(jax.random.key(seed), 3))
    return {
        "q": (3 * jax.random.normal(kq, (BATCH, HEADS, HEAD), jnp.float32)).astype(jnp.bfloat16),
        "k": jax.random.normal(kk, (BATCH, CACHE, KV_HEADS, HEAD), jnp.float32).astype(jnp.bfloat16),
        "v": jax.random.normal(kv, (BATCH, CACHE, KV_HEADS, HEAD), jnp.float32).astype(jnp.bfloat16),
    }


def einsum(form, a, b):
    return jnp.einsum(form, a.astype(jnp.float32), b.astype(jnp.float32))


def reference(q, k, v):
    grouped = q.reshape(BATCH, KV_HEADS, -1, HEAD)
    scores = einsum("bgsd,bugd->bgsu", grouped, k) * HEAD**-0.5
    weights = jax.nn.softmax(scores, -1).astype(jnp.bfloat16)
    return einsum("bgsu,bugd->bgsd", weights, v).astype(jnp.bfloat16).reshape(BATCH, HEADS, HEAD)
```

```python
import functools
import math

import jax
import jax.numpy as jnp
from jax import lax
from jax.experimental import pallas as pl
from jax.experimental.pallas import tpu as pltpu
from jax.sharding import PartitionSpec as P

SLOTS = 4
LAG_A = 4
LAG_B = 3
F32, BF16 = jnp.float32, jnp.bfloat16


def weights_of(q, keys, slot, scale):
    rows, depth = q.shape
    half, tokens = rows // 2, keys.shape[2]
    zero = jnp.zeros((half, depth), q.dtype)
    both = jnp.concatenate([jnp.concatenate([q[:half], zero], 1), jnp.concatenate([zero, q[half:]], 1)], 0)
    lane = lax.broadcasted_iota(jnp.int32, (tokens, rows), 1) % half
    scores = jnp.zeros((tokens, rows), F32)
    for pair in range(half):
        two = jnp.concatenate([keys[slot, pair], keys[slot, pair + half]], 1)
        got = lax.dot_general(two, both, (((1,), (1,)), ((), ())), preferred_element_type=F32)
        scores = jnp.where(lane == pair, got, scores)
    scores = scores * scale
    high = jnp.max(scores, 0, keepdims=True)
    weights = jnp.exp(scores - high)
    return weights.T.astype(BF16), high, jnp.sum(weights, 0, keepdims=True)


def seen_of(weights, values, slot):
    rows, depth, block = weights.shape[0], values.shape[3], 16
    row = lax.broadcasted_iota(jnp.int32, (block, depth), 0)
    seen = []
    for first in range(0, rows, block):
        some = weights[first : first + block]
        out = jnp.zeros((block, depth), F32)
        for j in range(block):
            out = jnp.where(row == j, jnp.dot(some, values[slot, first + j], preferred_element_type=F32), out)
        seen.append(out)
    return jnp.concatenate(seen, 0)


def rows_of(stats, head, which, count):
    rows = stats.shape[-1]
    place = lax.broadcasted_iota(jnp.int32, (8, rows), 0)
    out = jnp.broadcast_to(stats[head, 0, which : which + 1], (8, rows))
    for j in range(1, count):
        out = jnp.where(place == j, jnp.broadcast_to(stats[head, j, which : which + 1], (8, rows)), out)
    return out


def together(parts, stats, head, count, last):
    rows = parts.shape[2]
    place = lax.broadcasted_iota(jnp.int32, (8, stats.shape[-1]), 0)
    high = rows_of(stats, head, 0, count)
    top = jnp.max(high, 0, keepdims=True)
    scale = jnp.where(place < count, jnp.exp(high - top), 0.0)
    total = jnp.sum(jnp.where(place < count, rows_of(stats, head, 1, count), 0.0) * scale, 0, keepdims=True)
    if last:
        scale = scale / total
    columns = scale.T[:rows]
    out = parts[head, 0].astype(F32) * columns[:, 0:1]
    for j in range(1, count):
        out = out + parts[head, j].astype(F32) * columns[:, j : j + 1]
    return out, top, total


def kernel(n, inner, q_ref, k_ref, v_ref, o_ref, keys, values, held, held_stats, parts_a, stats_a, parts_b, stats_b, k_sem, v_sem, recv_a, recv_as, recv_b, recv_bs, sent):
    heads, rows, depth = q_ref.shape
    outer = n // inner
    scale = depth**-0.5
    me = lax.axis_index("sp")
    mine_a, mine_b = lax.rem(me, inner), me // inner
    peers_a = [mine_b * inner + lax.rem(mine_a + i, inner) for i in range(1, inner)]
    peers_b = [lax.rem(mine_b + i, outer) * inner + mine_a for i in range(1, outer)]

    def fetch(ref, buffer, sem, head):
        slot = lax.rem(head, SLOTS)
        return pltpu.make_async_copy(ref.at[:, head], buffer.at[slot], sem.at[slot])

    fetch_k = functools.partial(fetch, k_ref, keys, k_sem)
    fetch_v = functools.partial(fetch, v_ref, values, v_sem)
    for head in range(SLOTS):
        fetch_k(head).start()
        fetch_v(head).start()

    barrier = pltpu.get_barrier_semaphore()
    for peer in peers_a + peers_b:
        pl.semaphore_signal(barrier, inc=1, device_id={"sp": peer}, device_id_type=pl.DeviceIdType.MESH)
    pl.semaphore_wait(barrier, len(peers_a) + len(peers_b))

    def send(parts, stats, mine, peers, head, recv, recv_s, place):
        for peer in peers:
            for ref, sem, kind in ((parts, recv, 0), (stats, recv_s, 1)):
                pltpu.make_async_remote_copy(
                    src_ref=ref.at[head, mine],
                    dst_ref=ref.at[head, mine],
                    send_sem=sent.at[place + kind],
                    recv_sem=sem.at[head],
                    device_id={"sp": peer},
                    device_id_type=pl.DeviceIdType.MESH,
                ).start()

    def arrived(parts, stats, head, recv, recv_s, count):
        for ref, sem in ((parts, recv), (stats, recv_s)):
            some = ref.at[head, 0 : count - 1]
            pltpu.make_async_copy(some, some, sem.at[head]).wait()

    def send_a(head):
        send(parts_a, stats_a, mine_a, peers_a, head, recv_a, recv_as, 0)

    def send_b(head):
        send(parts_b, stats_b, mine_b, peers_b, head, recv_b, recv_bs, 2)

    def weigh(head):
        return weights_of(q_ref[head], keys, lax.rem(head, SLOTS), scale)

    def hold(weights, high, total):
        held[...] = weights
        held_stats[0:1] = high
        held_stats[1:2] = total

    def part(head, weights, stats):
        parts_a[head, mine_a] = seen_of(weights, values, lax.rem(head, SLOTS)).astype(BF16)
        stats_a[head, mine_a] = stats

    def block(head):
        seen, top, total = together(parts_a, stats_a, head, inner, False)
        parts_b[head, mine_b] = seen.astype(BF16)
        stats_b[head, mine_b, 0:1] = top
        stats_b[head, mine_b, 1:2] = total

    def final(head, to):
        o_ref[to] = together(parts_b, stats_b, head, outer, True)[0].astype(o_ref.dtype)

    for ref in (parts_a, stats_a, parts_b, stats_b):
        ref[heads] = jnp.zeros(ref.shape[1:], ref.dtype)

    fetch_k(0).wait()
    hold(*weigh(0))
    fetch_k(SLOTS).start()

    def step(i, _):
        a = i - 1 - LAG_A
        f = a - LAG_B

        @pl.when(a >= 0)
        def _():
            arrived(parts_a, stats_a, a, recv_a, recv_as, inner)

        @pl.when(f >= 0)
        def _():
            arrived(parts_b, stats_b, f, recv_b, recv_bs, outer)

        fetch_k(i).wait()
        fetch_v(i - 1).wait()
        weights, stats = held[...], held_stats[...]
        new = weigh(i)
        part(i - 1, weights, stats)
        block(jnp.where(a >= 0, a, heads))
        final(jnp.where(f >= 0, f, heads), jnp.maximum(f, 0))
        hold(*new)
        send_a(i - 1)

        @pl.when(a >= 0)
        def _():
            send_b(a)

        @pl.when(i + SLOTS < heads)
        def _():
            fetch_k(i + SLOTS).start()

        @pl.when(i - 1 + SLOTS < heads)
        def _():
            fetch_v(i - 1 + SLOTS).start()

        return 0

    lax.fori_loop(1, heads, step, 0)
    fetch_v(heads - 1).wait()
    part(heads - 1, held[...], held_stats[...])
    send_a(heads - 1)

    def drain_a(a, _):
        arrived(parts_a, stats_a, a, recv_a, recv_as, inner)
        block(a)
        send_b(a)
        return 0

    lax.fori_loop(heads - 1 - LAG_A, heads, drain_a, 0)

    def drain_b(f, _):
        arrived(parts_b, stats_b, f, recv_b, recv_bs, outer)
        final(f, f)
        return 0

    lax.fori_loop(heads - 1 - LAG_A - LAG_B, heads, drain_b, 0)
    for place, ref, count in ((0, parts_a, inner), (1, stats_a, inner), (2, parts_b, outer), (3, stats_b, outer)):
        some = ref.at[0:heads, 0 : count - 1]
        pltpu.make_async_copy(some, some, sent.at[place]).wait()


def solution(mesh):
    n = mesh.shape["sp"]
    inner = 2 * math.isqrt(n // 2)
    outer = n // inner

    def step(q, k, v):
        q, k, v = q.transpose(1, 0, 2), k.transpose(0, 2, 1, 3), v.transpose(0, 2, 1, 3)
        heads, rows, depth = q.shape
        tokens = k.shape[2]
        ring = (SLOTS, rows, tokens, depth)
        whole = pl.BlockSpec(memory_space=pltpu.VMEM)
        out = pl.pallas_call(
            functools.partial(kernel, n, inner),
            out_shape=jax.ShapeDtypeStruct(q.shape, q.dtype),
            in_specs=[whole, pl.BlockSpec(memory_space=pl.ANY), pl.BlockSpec(memory_space=pl.ANY)],
            out_specs=whole,
            scratch_shapes=[
                pltpu.VMEM(ring, k.dtype),
                pltpu.VMEM(ring, v.dtype),
                pltpu.VMEM((rows, tokens), BF16),
                pltpu.VMEM((2, rows), F32),
                pltpu.VMEM((heads + 1, inner, rows, depth), BF16),
                pltpu.VMEM((heads + 1, inner, 2, rows), F32),
                pltpu.VMEM((heads + 1, outer, rows, depth), BF16),
                pltpu.VMEM((heads + 1, outer, 2, rows), F32),
                pltpu.SemaphoreType.DMA((SLOTS,)),
                pltpu.SemaphoreType.DMA((SLOTS,)),
                pltpu.SemaphoreType.DMA((heads,)),
                pltpu.SemaphoreType.DMA((heads,)),
                pltpu.SemaphoreType.DMA((heads,)),
                pltpu.SemaphoreType.DMA((heads,)),
                pltpu.SemaphoreType.DMA((4,)),
            ],
            compiler_params=pltpu.CompilerParams(collective_id=0, has_side_effects=True, vmem_limit_bytes=56 * 2**20),
            name="attend",
        )(q, k, v)
        return out.transpose(1, 0, 2)

    return jax.shard_map(
        step,
        mesh=mesh,
        in_specs=(P("dp", None, None), P("dp", "sp", None, None), P("dp", "sp", None, None)),
        out_specs=P("dp", None, None),
        check_vma=False,
    )
```

```python
import functools
import math

import jax
import jax.numpy as jnp
from jax import lax
from jax.experimental import pallas as pl
from jax.experimental.pallas import tpu as pltpu
from jax.sharding import PartitionSpec as P

SLOTS = 16
GROUP = 2
CHUNK = 8
BULK = 4
TAIL = 2
LAG = 3
F32, BF16 = jnp.float32, jnp.bfloat16


def scores_of(q, keys, slot):
    rows, depth = q.shape
    half, tokens = rows // 2, keys.shape[2]
    zero = jnp.zeros((half, depth), q.dtype)
    both = jnp.concatenate([jnp.concatenate([q[:half], zero], 1), jnp.concatenate([zero, q[half:]], 1)], 0)
    lane = lax.broadcasted_iota(jnp.int32, (tokens, rows), 1) % half
    scores = jnp.zeros((tokens, rows), F32)
    for pair in range(half):
        two = jnp.concatenate([keys[slot, pair], keys[slot, pair + half]], 1)
        got = lax.dot_general(two, both, (((1,), (1,)), ((), ())), preferred_element_type=F32)
        scores = jnp.where(lane == pair, got, scores)
    return scores


def seen_of(weights, values, slot, first):
    row = lax.broadcasted_iota(jnp.int32, (weights.shape[0], values.shape[3]), 0)
    out = jnp.zeros(row.shape, F32)
    for j in range(weights.shape[0]):
        out = jnp.where(row == j, jnp.dot(weights, values[slot, first + j], preferred_element_type=F32), out)
    return out


def kernel(n, inner, q_ref, k_ref, v_ref, o_ref, ring, scores, weights, stats, share, mine, parts_a, parts_b, last_mine, last_a, last_b, ring_sem, recv_s, recv_a, recv_b, recv_la, recv_lb, sent):
    heads, rows, depth = q_ref.shape
    half, outer = rows // 2, n // inner
    bulks = heads // BULK - 1
    first_last = bulks * BULK
    per = CHUNK // GROUP
    scale = depth**-0.5
    me = lax.axis_index("sp")
    core = lax.rem(me, 2)
    mine_a, mine_b = lax.rem(me, inner), me // inner * 2 + core
    base_a, base_b = me // inner * inner, lax.rem(me, inner) // 2 * 2
    peers_s = [lax.rem(me + i, n) for i in range(1, n)]
    peers_a = [base_a + lax.rem(mine_a + i, inner) for i in range(1, inner)]
    places_b = [lax.rem(mine_b + i, 2 * outer) for i in range(1, 2 * outer)]
    peers_b = [place // 2 * inner + base_b + lax.rem(place, 2) for place in places_b]

    def fetch(ref, head, place):
        slot = lax.rem(place, SLOTS)
        return [
            pltpu.make_async_copy(ref.at[pl.ds(h * half, half), head], ring.at[slot, pl.ds(h * half, half)], ring_sem.at[slot, h])
            for h in range(2)
        ]

    def fetch_k(head):
        return fetch(k_ref, head, head)

    def fetch_v(head):
        return fetch(v_ref, head, heads + head)

    def fetch_next(place, count):
        @pl.when(place < heads)
        def _():
            for g in range(count):
                for copy in fetch_k(place + g):
                    copy.start()

        @pl.when((place >= heads) & (place < 2 * heads))
        def _():
            for g in range(count):
                for copy in fetch_v(place + g - heads):
                    copy.start()

    def wait(copies):
        for copy in copies:
            copy.wait()

    for head in range(SLOTS):
        for copy in fetch_k(head):
            copy.start()
    stats[...] = jnp.zeros(stats.shape, stats.dtype)
    parts_a[bulks] = jnp.zeros(parts_a.shape[1:], parts_a.dtype)

    barrier = pltpu.get_barrier_semaphore()
    for peer in peers_s:
        pl.semaphore_signal(barrier, inc=1, device_id={"sp": peer}, device_id_type=pl.DeviceIdType.MESH)

    def send(source, target, peer, recv, place):
        pltpu.make_async_remote_copy(
            src_ref=source, dst_ref=target, send_sem=sent.at[place], recv_sem=recv, device_id={"sp": peer}, device_id_type=pl.DeviceIdType.MESH
        ).start()

    def arrived(ref, index, recv):
        some = ref.at[index, 0 : ref.shape[1] - 1]
        pltpu.make_async_copy(some, some, recv.at[index]).wait()

    def send_s(chunk):
        for peer in peers_s:
            send(stats.at[chunk, me], stats.at[chunk, me], peer, recv_s.at[chunk], 0)

    def send_a(own, parts, group, recv, place):
        for i, peer in enumerate(peers_a):
            send(own.at[group, lax.rem(core + i + 1, 2)], parts.at[group, mine_a], peer, recv.at[group], place)

    def send_b(parts, group, recv, place):
        for peer in peers_b:
            send(parts.at[group, mine_b], parts.at[group, mine_b], peer, recv.at[group], place)

    def weigh(group):
        for g in range(GROUP):
            head = group * GROUP + g
            scaled = scores[g] * scale
            high = jnp.max(scaled, 0, keepdims=True)
            w = jnp.exp(scaled - high)
            weights[head] = w.T.astype(BF16)
            chunk, j = head // CHUNK, lax.rem(head, CHUNK)
            stats[chunk, me, 0, pl.ds(j, 1)] = high
            stats[chunk, me, 1, pl.ds(j, 1)] = jnp.sum(w, 0, keepdims=True)

    def score(group):
        new = []
        for g in range(GROUP):
            head = group * GROUP + g
            new.append(scores_of(q_ref[head], ring, lax.rem(head, SLOTS)))
        for g in range(GROUP):
            scores[g] = new[g]

    def shares(chunk):
        top = stats[chunk, 0, 0]
        for j in range(1, n):
            top = jnp.maximum(top, stats[chunk, j, 0])
        total = stats[chunk, 0, 1] * jnp.exp(stats[chunk, 0, 0] - top)
        for j in range(1, n):
            total = total + stats[chunk, j, 1] * jnp.exp(stats[chunk, j, 0] - top)
        columns = (jnp.exp(stats[chunk, me, 0] - top) / total).T
        for j in range(CHUNK):
            share[chunk * CHUNK + j] = jnp.broadcast_to(columns[:, j : j + 1], (rows, depth))

    def part(own, parts, group, g, head, h):
        at = slice(h * half, (h + 1) * half)
        seen = (seen_of(weights[head, at], ring, lax.rem(heads + head, SLOTS), h * half) * share[head, at]).astype(BF16)
        own[group, h, g] = seen
        return seen

    def keep(parts, group, g, seen):
        parts[group, mine_a, g] = jnp.where(core == 0, seen[0], seen[1])

    def block(parts, to, group, to_group, count):
        for g in range(count):
            out = parts[group, 0, g].astype(F32)
            for j in range(1, inner):
                out = out + parts[group, j, g].astype(F32)
            to[to_group, mine_b, g] = out.astype(BF16)

    def final(parts, group, head, count):
        for g in range(count):
            for h in range(2):
                out = parts[group, h, g].astype(F32)
                for j in range(1, outer):
                    out = out + parts[group, 2 * j + h, g].astype(F32)
                o_ref[head + g, h * half : (h + 1) * half] = out.astype(o_ref.dtype)

    for g in range(GROUP):
        wait(fetch_k(g))
    score(0)
    fetch_next(SLOTS, GROUP)

    def keys_step(i, _):
        for g in range(GROUP):
            wait(fetch_k(i * GROUP + g))
        weigh(i - 1)
        score(i)
        fetch_next(i * GROUP + SLOTS, GROUP)

        @pl.when(i == per)
        def _():
            pl.semaphore_wait(barrier, n - 1)

        @pl.when(lax.rem(i, per) == 0)
        def _():
            send_s(i // per - 1)

        return 0

    lax.fori_loop(1, heads // GROUP, keys_step, 0)
    weigh(heads // GROUP - 1)
    send_s((heads - 1) // CHUNK)

    def values_step(i, _):
        a = i - LAG

        @pl.when(lax.rem(i, CHUNK // BULK) == 0)
        def _():
            arrived(stats, i // (CHUNK // BULK), recv_s)
            shares(i // (CHUNK // BULK))

        @pl.when(a >= 0)
        def _():
            arrived(parts_a, a, recv_a)

        for g in range(BULK):
            wait(fetch_v(i * BULK + g))
        for g in range(BULK):
            keep(parts_a, i, g, [part(mine, parts_a, i, g, i * BULK + g, h) for h in range(2)])
        block(parts_a, parts_b, jnp.where(a >= 0, a, bulks), jnp.where(a >= 0, a, bulks), BULK)
        send_a(mine, parts_a, i, recv_a, 1)

        @pl.when(a >= 0)
        def _():
            send_b(parts_b, a, recv_b, 2)

        fetch_next(heads + i * BULK + SLOTS, BULK)
        return 0

    lax.fori_loop(0, bulks, values_step, 0)

    def block_bulk(a):
        arrived(parts_a, a, recv_a)
        block(parts_a, parts_b, a, a, BULK)
        send_b(parts_b, a, recv_b, 2)

    def final_bulk(f):
        arrived(parts_b, f, recv_b)
        final(parts_b, f, f * BULK, BULK)

    arrived(stats, first_last // CHUNK, recv_s)
    shares(first_last // CHUNK)
    waiting = list(range(bulks - LAG, bulks))
    for t in range(BULK // TAIL):
        for g in range(TAIL):
            head = first_last + t * TAIL + g
            if head < heads - 1:
                wait(fetch_v(head))
            seen = []
            for h in range(2):
                if head == heads - 1:
                    fetch_v(head)[h].wait()
                seen.append(part(last_mine, last_a, t, g, head, h))
            keep(last_a, t, g, seen)
        send_a(last_mine, last_a, t, recv_la, 3)
        if t == 0:
            block_bulk(waiting.pop(0))
    for a in waiting:
        block_bulk(a)
    for f in range(bulks - LAG):
        final_bulk(f)
    for t in range(BULK // TAIL):
        arrived(last_a, t, recv_la)
        block(last_a, last_b, t, t, TAIL)
        send_b(last_b, t, recv_lb, 4)
    for f in range(bulks - LAG, bulks):
        final_bulk(f)
    for t in range(BULK // TAIL):
        arrived(last_b, t, recv_lb)
        final(last_b, t, first_last + t * TAIL, TAIL)
    every = (stats.at[:, 0 : n - 1], parts_a.at[0:bulks, 0 : inner - 1], parts_b.at[0:bulks, 0 : 2 * outer - 1], last_a.at[:, 0 : inner - 1], last_b.at[:, 0 : 2 * outer - 1])
    for place, some in enumerate(every):
        pltpu.make_async_copy(some, some, sent.at[place]).wait()


def solution(mesh):
    n = mesh.shape["sp"]
    inner = 2 * math.isqrt(n // 2)
    outer = n // inner

    def step(q, k, v):
        q, k, v = q.transpose(1, 0, 2), k.transpose(0, 2, 1, 3), v.transpose(0, 2, 1, 3)
        heads, rows, depth = q.shape
        tokens, half = k.shape[2], rows // 2
        chunks, bulks, lasts = -(-heads // CHUNK), heads // BULK - 1, BULK // TAIL
        whole = pl.BlockSpec(memory_space=pltpu.VMEM)
        out = pl.pallas_call(
            functools.partial(kernel, n, inner),
            out_shape=pltpu.VMEM(q.shape, q.dtype),
            in_specs=[whole, pl.BlockSpec(memory_space=pl.ANY), pl.BlockSpec(memory_space=pl.ANY)],
            out_specs=whole,
            scratch_shapes=[
                pltpu.VMEM((SLOTS, rows, tokens, depth), k.dtype),
                pltpu.VMEM((GROUP, tokens, rows), F32),
                pltpu.VMEM((heads, rows, tokens), BF16),
                pltpu.VMEM((chunks, n, 2, CHUNK, rows), F32),
                pltpu.VMEM((chunks * CHUNK, rows, depth), F32),
                pltpu.VMEM((bulks, 2, BULK, half, depth), BF16),
                pltpu.VMEM((bulks + 1, inner, BULK, half, depth), BF16),
                pltpu.VMEM((bulks + 1, 2 * outer, BULK, half, depth), BF16),
                pltpu.VMEM((lasts, 2, TAIL, half, depth), BF16),
                pltpu.VMEM((lasts, inner, TAIL, half, depth), BF16),
                pltpu.VMEM((lasts, 2 * outer, TAIL, half, depth), BF16),
                pltpu.SemaphoreType.DMA((SLOTS, 2)),
                pltpu.SemaphoreType.DMA((chunks,)),
                pltpu.SemaphoreType.DMA((bulks,)),
                pltpu.SemaphoreType.DMA((bulks,)),
                pltpu.SemaphoreType.DMA((lasts,)),
                pltpu.SemaphoreType.DMA((lasts,)),
                pltpu.SemaphoreType.DMA((5,)),
            ],
            compiler_params=pltpu.CompilerParams(collective_id=0, has_side_effects=True, vmem_limit_bytes=56 * 2**20),
            name="attend",
        )(q, k, v)
        return out.transpose(1, 0, 2)

    return jax.shard_map(
        step,
        mesh=mesh,
        in_specs=(P("dp", None, None), P("dp", "sp", None, None), P("dp", "sp", None, None)),
        out_specs=P("dp", None, None),
        check_vma=False,
    )
```

```python
import functools
import math

import jax
import jax.numpy as jnp
from jax import lax
from jax.experimental import pallas as pl
from jax.experimental.pallas import tpu as pltpu
from jax.sharding import PartitionSpec as P

SLOTS = 16
GROUP = 2
CHUNK = 8
BULK = 4
TAIL = 2
PIECES = 2
LAG = 3
F32, BF16 = jnp.float32, jnp.bfloat16


def scores_of(q, keys, slot):
    rows, depth = q.shape
    half, tokens = rows // 2, keys.shape[2]
    zero = jnp.zeros((half, depth), q.dtype)
    both = jnp.concatenate([jnp.concatenate([q[:half], zero], 1), jnp.concatenate([zero, q[half:]], 1)], 0)
    lane = lax.broadcasted_iota(jnp.int32, (tokens, rows), 1) % half
    scores = jnp.zeros((tokens, rows), F32)
    for pair in range(half):
        two = jnp.concatenate([keys[slot, pair], keys[slot, pair + half]], 1)
        got = lax.dot_general(two, both, (((1,), (1,)), ((), ())), preferred_element_type=F32)
        scores = jnp.where(lane == pair, got, scores)
    return scores


def seen_of(weights, values, slot, first, ready):
    row = lax.broadcasted_iota(jnp.int32, (weights.shape[0], values.shape[3]), 0)
    out = jnp.zeros(row.shape, F32)
    for j in range(weights.shape[0]):
        ready(first + j)
        out = jnp.where(row == j, jnp.dot(weights, values[slot, first + j], preferred_element_type=F32), out)
    return out


def kernel(n, inner, q_hbm, k_ref, v_ref, o_ref, q_ref, ring, scores, weights, stats, share, mine, parts_a, parts_b, last_mine, last_a, last_b, q_sem, ring_sem, recv_s, recv_a, recv_b, recv_la, recv_lb, sent):
    heads, rows, depth = q_ref.shape
    half, outer, piece = rows // 2, n // inner, rows // PIECES
    bulks = heads // BULK - 1
    first_last = bulks * BULK
    per = CHUNK // GROUP
    scale = depth**-0.5
    me = lax.axis_index("sp")
    core = lax.rem(me, 2)
    mine_a, mine_b = lax.rem(me, inner), me // inner * 2 + core
    base_a, base_b = me // inner * inner, lax.rem(me, inner) // 2 * 2
    def far_first(count):
        return sorted(range(1, count), key=lambda i: -min(i, count - i))

    peers_s = [lax.rem(me + i, n) for i in range(1, n)]
    peers_a = [(i, base_a + lax.rem(mine_a + i, inner)) for i in far_first(inner)]
    places_b = [lax.rem(mine_b + i, 2 * outer) for i in far_first(2 * outer)]
    peers_b = [place // 2 * inner + base_b + lax.rem(place, 2) for place in places_b]

    def fetch(ref, head, place):
        slot = lax.rem(place, SLOTS)
        return [
            pltpu.make_async_copy(ref.at[pl.ds(p * piece, piece), head], ring.at[slot, pl.ds(p * piece, piece)], ring_sem.at[slot, p])
            for p in range(PIECES)
        ]

    def fetch_k(head):
        return fetch(k_ref, head, head)

    def fetch_v(head):
        return fetch(v_ref, head, heads + head)

    def fetch_next(place, count):
        @pl.when(place < heads)
        def _():
            for g in range(count):
                for copy in fetch_k(place + g):
                    copy.start()

        @pl.when((place >= heads) & (place < 2 * heads))
        def _():
            for g in range(count):
                for copy in fetch_v(place + g - heads):
                    copy.start()

    def wait(copies):
        for copy in copies:
            copy.wait()

    fetch_q = pltpu.make_async_copy(q_hbm, q_ref, q_sem)
    fetch_q.start()
    for head in range(GROUP):
        for copy in fetch_k(head):
            copy.start()
    stats[...] = jnp.zeros(stats.shape, stats.dtype)
    parts_a[bulks] = jnp.zeros(parts_a.shape[1:], parts_a.dtype)

    barrier = pltpu.get_barrier_semaphore()
    for peer in peers_s:
        pl.semaphore_signal(barrier, inc=1, device_id={"sp": peer}, device_id_type=pl.DeviceIdType.MESH)
    for head in range(GROUP, SLOTS):
        for copy in fetch_k(head):
            copy.start()

    def send(source, target, peer, recv, place):
        pltpu.make_async_remote_copy(
            src_ref=source, dst_ref=target, send_sem=sent.at[place], recv_sem=recv, device_id={"sp": peer}, device_id_type=pl.DeviceIdType.MESH
        ).start()

    def arrived(ref, index, recv):
        some = ref.at[index, 0 : ref.shape[1] - 1]
        pltpu.make_async_copy(some, some, recv.at[index]).wait()

    def send_s(chunk):
        for peer in peers_s:
            send(stats.at[chunk, me], stats.at[chunk, me], peer, recv_s.at[chunk], 0)

    def send_a(own, parts, group, recv, place):
        for i, peer in peers_a:
            send(own.at[group, lax.rem(core + i, 2)], parts.at[group, mine_a], peer, recv.at[group], place)

    def send_b(parts, group, recv, place):
        for peer in peers_b:
            send(parts.at[group, mine_b], parts.at[group, mine_b], peer, recv.at[group], place)

    def weigh(group):
        for g in range(GROUP):
            head = group * GROUP + g
            scaled = scores[g] * scale
            high = jnp.max(scaled, 0, keepdims=True)
            w = jnp.exp(scaled - high)
            weights[head] = w.T.astype(BF16)
            chunk, j = head // CHUNK, lax.rem(head, CHUNK)
            stats[chunk, me, 0, pl.ds(j, 1)] = high
            stats[chunk, me, 1, pl.ds(j, 1)] = jnp.sum(w, 0, keepdims=True)

    def score(group):
        new = []
        for g in range(GROUP):
            head = group * GROUP + g
            new.append(scores_of(q_ref[head], ring, lax.rem(head, SLOTS)))
        for g in range(GROUP):
            scores[g] = new[g]

    def shares(chunk):
        top = stats[chunk, 0, 0]
        for j in range(1, n):
            top = jnp.maximum(top, stats[chunk, j, 0])
        total = stats[chunk, 0, 1] * jnp.exp(stats[chunk, 0, 0] - top)
        for j in range(1, n):
            total = total + stats[chunk, j, 1] * jnp.exp(stats[chunk, j, 0] - top)
        columns = (jnp.exp(stats[chunk, me, 0] - top) / total).T
        for j in range(CHUNK):
            share[chunk * CHUNK + j] = jnp.broadcast_to(columns[:, j : j + 1], (rows, depth))

    def part(own, group, g, head, h, ready=lambda row: None):
        at = slice(h * half, (h + 1) * half)
        seen = (seen_of(weights[head, at], ring, lax.rem(heads + head, SLOTS), h * half, ready) * share[head, at]).astype(BF16)
        own[group, h, g] = seen
        return seen

    def keep(parts, group, g, seen):
        parts[group, mine_a, g] = jnp.where(core == 0, seen[0], seen[1])

    def block(parts, to, group, to_group, count):
        for g in range(count):
            out = parts[group, 0, g].astype(F32)
            for j in range(1, inner):
                out = out + parts[group, j, g].astype(F32)
            to[to_group, mine_b, g] = out.astype(BF16)

    def final(parts, group, head, count):
        for g in range(count):
            for h in range(2):
                out = parts[group, h, g].astype(F32)
                for j in range(1, outer):
                    out = out + parts[group, 2 * j + h, g].astype(F32)
                o_ref[head + g, h * half : (h + 1) * half] = out.astype(o_ref.dtype)

    fetch_q.wait()
    for g in range(GROUP):
        wait(fetch_k(g))
    score(0)
    fetch_next(SLOTS, GROUP)

    def keys_step(i, _):
        for g in range(GROUP):
            wait(fetch_k(i * GROUP + g))
        weigh(i - 1)
        score(i)
        fetch_next(i * GROUP + SLOTS, GROUP)

        @pl.when(i == per)
        def _():
            pl.semaphore_wait(barrier, n - 1)

        @pl.when(lax.rem(i, per) == 0)
        def _():
            send_s(i // per - 1)

        return 0

    lax.fori_loop(1, heads // GROUP, keys_step, 0)
    weigh(heads // GROUP - 1)
    send_s((heads - 1) // CHUNK)

    def values_step(i, _):
        a = i - LAG

        @pl.when(lax.rem(i, CHUNK // BULK) == 0)
        def _():
            arrived(stats, i // (CHUNK // BULK), recv_s)
            shares(i // (CHUNK // BULK))

        @pl.when(a >= 0)
        def _():
            arrived(parts_a, a, recv_a)

        for g in range(BULK):
            wait(fetch_v(i * BULK + g))
        for g in range(BULK):
            keep(parts_a, i, g, [part(mine, i, g, i * BULK + g, h) for h in range(2)])
        block(parts_a, parts_b, jnp.where(a >= 0, a, bulks), jnp.where(a >= 0, a, bulks), BULK)
        send_a(mine, parts_a, i, recv_a, 1)

        @pl.when(a >= 0)
        def _():
            send_b(parts_b, a, recv_b, 2)

        fetch_next(heads + i * BULK + SLOTS, BULK)
        return 0

    lax.fori_loop(0, bulks, values_step, 0)

    def block_bulk(a):
        arrived(parts_a, a, recv_a)
        block(parts_a, parts_b, a, a, BULK)
        send_b(parts_b, a, recv_b, 2)

    def final_bulk(f):
        arrived(parts_b, f, recv_b)
        final(parts_b, f, f * BULK, BULK)

    arrived(stats, first_last // CHUNK, recv_s)
    shares(first_last // CHUNK)
    waiting = list(range(bulks - LAG, bulks))
    for t in range(BULK // TAIL):
        for g in range(TAIL):
            head = first_last + t * TAIL + g
            copies = fetch_v(head)
            if head < heads - 1:
                wait(copies)

            def ready(row):
                if head == heads - 1 and row % piece == 0:
                    copies[row // piece].wait()

            keep(last_a, t, g, [part(last_mine, t, g, head, h, ready) for h in range(2)])
        send_a(last_mine, last_a, t, recv_la, 3)
        if t == 0:
            block_bulk(waiting.pop(0))
    for a in waiting:
        block_bulk(a)
    for f in range(bulks - LAG):
        final_bulk(f)
    for t in range(BULK // TAIL):
        arrived(last_a, t, recv_la)
        block(last_a, last_b, t, t, TAIL)
        send_b(last_b, t, recv_lb, 4)
    for f in range(bulks - LAG, bulks):
        final_bulk(f)
    for t in range(BULK // TAIL):
        arrived(last_b, t, recv_lb)
        final(last_b, t, first_last + t * TAIL, TAIL)
    every = (stats.at[:, 0 : n - 1], parts_a.at[0:bulks, 0 : inner - 1], parts_b.at[0:bulks, 0 : 2 * outer - 1], last_a.at[:, 0 : inner - 1], last_b.at[:, 0 : 2 * outer - 1])
    for place, some in enumerate(every):
        pltpu.make_async_copy(some, some, sent.at[place]).wait()


def solution(mesh):
    n = mesh.shape["sp"]
    inner = 2 * math.isqrt(n // 2)
    outer = n // inner

    def step(q, k, v):
        q, k, v = q.transpose(1, 0, 2), k.transpose(0, 2, 1, 3), v.transpose(0, 2, 1, 3)
        heads, rows, depth = q.shape
        tokens, half = k.shape[2], rows // 2
        chunks, bulks, lasts = -(-heads // CHUNK), heads // BULK - 1, BULK // TAIL
        whole = pl.BlockSpec(memory_space=pltpu.VMEM)
        out = pl.pallas_call(
            functools.partial(kernel, n, inner),
            out_shape=pltpu.VMEM(q.shape, q.dtype),
            in_specs=[pl.BlockSpec(memory_space=pl.ANY)] * 3,
            out_specs=whole,
            scratch_shapes=[
                pltpu.VMEM(q.shape, q.dtype),
                pltpu.VMEM((SLOTS, rows, tokens, depth), k.dtype),
                pltpu.VMEM((GROUP, tokens, rows), F32),
                pltpu.VMEM((heads, rows, tokens), BF16),
                pltpu.VMEM((chunks, n, 2, CHUNK, rows), F32),
                pltpu.VMEM((chunks * CHUNK, rows, depth), F32),
                pltpu.VMEM((bulks, 2, BULK, half, depth), BF16),
                pltpu.VMEM((bulks + 1, inner, BULK, half, depth), BF16),
                pltpu.VMEM((bulks + 1, 2 * outer, BULK, half, depth), BF16),
                pltpu.VMEM((lasts, 2, TAIL, half, depth), BF16),
                pltpu.VMEM((lasts, inner, TAIL, half, depth), BF16),
                pltpu.VMEM((lasts, 2 * outer, TAIL, half, depth), BF16),
                pltpu.SemaphoreType.DMA,
                pltpu.SemaphoreType.DMA((SLOTS, PIECES)),
                pltpu.SemaphoreType.DMA((chunks,)),
                pltpu.SemaphoreType.DMA((bulks,)),
                pltpu.SemaphoreType.DMA((bulks,)),
                pltpu.SemaphoreType.DMA((lasts,)),
                pltpu.SemaphoreType.DMA((lasts,)),
                pltpu.SemaphoreType.DMA((5,)),
            ],
            compiler_params=pltpu.CompilerParams(collective_id=0, has_side_effects=True, vmem_limit_bytes=56 * 2**20),
            name="attend",
        )(q, k, v)
        return out.transpose(1, 0, 2)

    return jax.shard_map(
        step,
        mesh=mesh,
        in_specs=(P("dp", None, None), P("dp", "sp", None, None), P("dp", "sp", None, None)),
        out_specs=P("dp", None, None),
        check_vma=False,
    )
```

```python
import functools
import math

import jax
import jax.numpy as jnp
from jax import lax
from jax.experimental import pallas as pl
from jax.experimental.pallas import tpu as pltpu
from jax.sharding import PartitionSpec as P

SLOTS = 16
GROUP = 2
CHUNK = 8
BULK = 4
TAIL = 2
LAST = 8
PIECES = 2
F32, BF16 = jnp.float32, jnp.bfloat16


def scores_of(q, keys, slot):
    rows, depth = q.shape
    half, tokens = rows // 2, keys.shape[2]
    zero = jnp.zeros((half, depth), q.dtype)
    both = jnp.concatenate([jnp.concatenate([q[:half], zero], 1), jnp.concatenate([zero, q[half:]], 1)], 0)
    lane = lax.broadcasted_iota(jnp.int32, (tokens, rows), 1) % half
    scores = jnp.zeros((tokens, rows), F32)
    for pair in range(half):
        two = jnp.concatenate([keys[slot, pair], keys[slot, pair + half]], 1)
        got = lax.dot_general(two, both, (((1,), (1,)), ((), ())), preferred_element_type=F32)
        scores = jnp.where(lane == pair, got, scores)
    return scores


def seen_of(weights, values, slot, first, ready):
    row = lax.broadcasted_iota(jnp.int32, (weights.shape[0], values.shape[3]), 0)
    out = jnp.zeros(row.shape, F32)
    for j in range(weights.shape[0]):
        ready(first + j)
        out = jnp.where(row == j, jnp.dot(weights, values[slot, first + j], preferred_element_type=F32), out)
    return out


def kernel(n, inner, q_hbm, k_ref, v_ref, o_ref, q_ref, ring, scores, weights, stats, share, mine, parts_a, parts_b, last_mine, last_a, last_b, q_sem, ring_sem, recv_s, recv_a, recv_b, recv_la, recv_lb, sent):
    heads, rows, depth = q_ref.shape
    half, outer, piece = rows // 2, n // inner, rows // PIECES
    bulks, lasts = (heads - LAST) // BULK, LAST // TAIL
    first_last = bulks * BULK
    per = CHUNK // GROUP
    scale = depth**-0.5
    me = lax.axis_index("sp")
    core = lax.rem(me, 2)
    mine_a, mine_b = lax.rem(me, inner), me // inner * 2 + core
    base_a, base_b = me // inner * inner, lax.rem(me, inner) // 2 * 2
    def far_first(count):
        return sorted(range(1, count), key=lambda i: -min(i // 2 * 2, count - i // 2 * 2))

    peers_s = [lax.rem(me + i, n) for i in range(1, n)]
    peers_a = [(i, base_a + lax.rem(mine_a + i, inner)) for i in far_first(inner)]
    places_b = [lax.rem(mine_b + i, 2 * outer) for i in far_first(2 * outer)]
    peers_b = [place // 2 * inner + base_b + lax.rem(place, 2) for place in places_b]

    def fetch(ref, head, place):
        slot = lax.rem(place, SLOTS)
        return [
            pltpu.make_async_copy(ref.at[pl.ds(p * piece, piece), head], ring.at[slot, pl.ds(p * piece, piece)], ring_sem.at[slot, p])
            for p in range(PIECES)
        ]

    def fetch_k(head):
        return fetch(k_ref, head, head)

    def fetch_v(head):
        return fetch(v_ref, head, heads + head)

    def fetch_next(place, count):
        @pl.when(place < heads)
        def _():
            for g in range(count):
                for copy in fetch_k(place + g):
                    copy.start()

        @pl.when((place >= heads) & (place < 2 * heads))
        def _():
            for g in range(count):
                for copy in fetch_v(place + g - heads):
                    copy.start()

    def wait(copies):
        for copy in copies:
            copy.wait()

    fetch_q = pltpu.make_async_copy(q_hbm, q_ref, q_sem)
    fetch_q.start()
    for head in range(GROUP):
        for copy in fetch_k(head):
            copy.start()
    stats[...] = jnp.zeros(stats.shape, stats.dtype)

    barrier = pltpu.get_barrier_semaphore()
    for peer in peers_s:
        pl.semaphore_signal(barrier, inc=1, device_id={"sp": peer}, device_id_type=pl.DeviceIdType.MESH)
    for head in range(GROUP, SLOTS):
        for copy in fetch_k(head):
            copy.start()

    def send(source, target, peer, recv, place):
        pltpu.make_async_remote_copy(
            src_ref=source, dst_ref=target, send_sem=sent.at[place], recv_sem=recv, device_id={"sp": peer}, device_id_type=pl.DeviceIdType.MESH
        ).start()

    def arrived(ref, index, recv):
        some = ref.at[index, 0 : ref.shape[1] - 1]
        pltpu.make_async_copy(some, some, recv.at[index]).wait()

    def send_s(chunk):
        for peer in peers_s:
            send(stats.at[chunk, me], stats.at[chunk, me], peer, recv_s.at[chunk], 0)

    def send_a(own, parts, group, recv, place):
        for i, peer in peers_a:
            send(own.at[group, lax.rem(core + i, 2)], parts.at[group, mine_a], peer, recv.at[group], place)

    def send_b(parts, group, recv, place):
        for peer in peers_b:
            send(parts.at[group, mine_b], parts.at[group, mine_b], peer, recv.at[group], place)

    def weigh(group):
        for g in range(GROUP):
            head = group * GROUP + g
            scaled = scores[g] * scale
            high = jnp.max(scaled, 0, keepdims=True)
            w = jnp.exp(scaled - high)
            weights[head] = w.T.astype(BF16)
            chunk, j = head // CHUNK, lax.rem(head, CHUNK)
            stats[chunk, me, pl.ds(j, 1)] = jnp.concatenate([high, jnp.sum(w, 0, keepdims=True)], 1)

    def score(group):
        new = []
        for g in range(GROUP):
            head = group * GROUP + g
            new.append(scores_of(q_ref[head], ring, lax.rem(head, SLOTS)))
        for g in range(GROUP):
            scores[g] = new[g]

    def shares(chunk):
        top = stats[chunk, 0, :, :rows]
        for j in range(1, n):
            top = jnp.maximum(top, stats[chunk, j, :, :rows])
        total = jnp.zeros(top.shape, F32)
        for j in range(n):
            total = total + stats[chunk, j, :, rows:] * jnp.exp(stats[chunk, j, :, :rows] - top)
        columns = (jnp.exp(stats[chunk, me, :, :rows] - top) / total).T
        for j in range(CHUNK):
            share[chunk * CHUNK + j] = jnp.broadcast_to(columns[:, j : j + 1], (rows, depth))

    def part(own, group, g, head, h, ready=lambda row: None):
        at = slice(h * half, (h + 1) * half)
        seen = (seen_of(weights[head, at], ring, lax.rem(heads + head, SLOTS), h * half, ready) * share[head, at]).astype(BF16)
        own[group, h, g] = seen
        return seen

    def keep(parts, group, g, seen):
        parts[group, mine_a, g] = jnp.where(core == 0, seen[0], seen[1])

    def block(parts, to, group, to_group, count):
        for g in range(count):
            out = parts[group, 0, g].astype(F32)
            for j in range(1, inner):
                out = out + parts[group, j, g].astype(F32)
            to[to_group, mine_b, g] = out.astype(BF16)

    def final(parts, group, head, count):
        for g in range(count):
            for h in range(2):
                out = parts[group, h, g].astype(F32)
                for j in range(1, outer):
                    out = out + parts[group, 2 * j + h, g].astype(F32)
                o_ref[head + g, h * half : (h + 1) * half] = out.astype(o_ref.dtype)

    fetch_q.wait()
    for g in range(GROUP):
        wait(fetch_k(g))
    score(0)
    fetch_next(SLOTS, GROUP)

    def keys_step(i, _):
        for g in range(GROUP):
            wait(fetch_k(i * GROUP + g))
        weigh(i - 1)
        score(i)
        fetch_next(i * GROUP + SLOTS, GROUP)

        @pl.when(i == per)
        def _():
            pl.semaphore_wait(barrier, n - 1)

        @pl.when(lax.rem(i, per) == 0)
        def _():
            send_s(i // per - 1)

        return 0

    lax.fori_loop(1, heads // GROUP, keys_step, 0)
    weigh(heads // GROUP - 1)
    send_s((heads - 1) // CHUNK)

    def ready_s(head):
        arrived(stats, head // CHUNK, recv_s)
        shares(head // CHUNK)

    def values_step(i, _):
        @pl.when(lax.rem(i, CHUNK // BULK) == 0)
        def _():
            ready_s(i * BULK)

        for g in range(BULK):
            wait(fetch_v(i * BULK + g))
        for g in range(BULK):
            keep(parts_a, i, g, [part(mine, i, g, i * BULK + g, h) for h in range(2)])
        send_a(mine, parts_a, i, recv_a, 1)
        fetch_next(heads + i * BULK + SLOTS, BULK)
        return 0

    lax.fori_loop(0, bulks, values_step, 0)

    def block_bulk(a):
        arrived(parts_a, a, recv_a)
        block(parts_a, parts_b, a, a, BULK)
        send_b(parts_b, a, recv_b, 2)

    def final_bulk(f):
        arrived(parts_b, f, recv_b)
        final(parts_b, f, f * BULK, BULK)

    def block_last(t):
        arrived(last_a, t, recv_la)
        block(last_a, last_b, t, t, TAIL)
        send_b(last_b, t, recv_lb, 4)

    def final_last(t):
        arrived(last_b, t, recv_lb)
        final(last_b, t, first_last + t * TAIL, TAIL)

    for t in range(lasts):
        for g in range(TAIL):
            head = first_last + t * TAIL + g
            if head % CHUNK == 0:
                ready_s(head)
            copies = fetch_v(head)
            if head < heads - 1:
                wait(copies)

            def ready(row):
                if head == heads - 1 and row % piece == 0:
                    copies[row // piece].wait()

            keep(last_a, t, g, [part(last_mine, t, g, head, h, ready) for h in range(2)])
        send_a(last_mine, last_a, t, recv_la, 3)
        if t < bulks - 1:
            block_bulk(t)
    for a in range(min(lasts, bulks - 1), bulks):
        block_bulk(a)
    for t in range(lasts):
        block_last(t)
    for f in range(bulks):
        final_bulk(f)
    for t in range(lasts):
        final_last(t)
    every = (stats.at[:, 0 : n - 1], parts_a.at[:, 0 : inner - 1], parts_b.at[:, 0 : 2 * outer - 1], last_a.at[:, 0 : inner - 1], last_b.at[:, 0 : 2 * outer - 1])
    for place, some in enumerate(every):
        pltpu.make_async_copy(some, some, sent.at[place]).wait()


def solution(mesh):
    n = mesh.shape["sp"]
    inner = 2 * math.isqrt(n // 2)
    outer = n // inner

    def step(q, k, v):
        q, k, v = q.transpose(1, 0, 2), k.transpose(0, 2, 1, 3), v.transpose(0, 2, 1, 3)
        heads, rows, depth = q.shape
        tokens, half = k.shape[2], rows // 2
        chunks, bulks, lasts = -(-heads // CHUNK), (heads - LAST) // BULK, LAST // TAIL
        whole = pl.BlockSpec(memory_space=pltpu.VMEM)
        out = pl.pallas_call(
            functools.partial(kernel, n, inner),
            out_shape=pltpu.VMEM(q.shape, q.dtype),
            in_specs=[pl.BlockSpec(memory_space=pl.ANY)] * 3,
            out_specs=whole,
            scratch_shapes=[
                pltpu.VMEM(q.shape, q.dtype),
                pltpu.VMEM((SLOTS, rows, tokens, depth), k.dtype),
                pltpu.VMEM((GROUP, tokens, rows), F32),
                pltpu.VMEM((heads, rows, tokens), BF16),
                pltpu.VMEM((chunks, n, CHUNK, 2 * rows), F32),
                pltpu.VMEM((chunks * CHUNK, rows, depth), F32),
                pltpu.VMEM((bulks, 2, BULK, half, depth), BF16),
                pltpu.VMEM((bulks, inner, BULK, half, depth), BF16),
                pltpu.VMEM((bulks, 2 * outer, BULK, half, depth), BF16),
                pltpu.VMEM((lasts, 2, TAIL, half, depth), BF16),
                pltpu.VMEM((lasts, inner, TAIL, half, depth), BF16),
                pltpu.VMEM((lasts, 2 * outer, TAIL, half, depth), BF16),
                pltpu.SemaphoreType.DMA,
                pltpu.SemaphoreType.DMA((SLOTS, PIECES)),
                pltpu.SemaphoreType.DMA((chunks,)),
                pltpu.SemaphoreType.DMA((bulks,)),
                pltpu.SemaphoreType.DMA((bulks,)),
                pltpu.SemaphoreType.DMA((lasts,)),
                pltpu.SemaphoreType.DMA((lasts,)),
                pltpu.SemaphoreType.DMA((5,)),
            ],
            compiler_params=pltpu.CompilerParams(collective_id=0, has_side_effects=True, vmem_limit_bytes=56 * 2**20),
            name="attend",
        )(q, k, v)
        return out.transpose(1, 0, 2)

    return jax.shard_map(
        step,
        mesh=mesh,
        in_specs=(P("dp", None, None), P("dp", "sp", None, None), P("dp", "sp", None, None)),
        out_specs=P("dp", None, None),
        check_vma=False,
    )
```

```python
import functools
import math

import jax
import jax.numpy as jnp
from jax import lax
from jax.experimental import pallas as pl
from jax.experimental.pallas import tpu as pltpu
from jax.sharding import PartitionSpec as P

SLOTS = 16
GROUP = 2
CHUNK = 8
BULK = 4
TAIL = 2
LAST = 8
PIECES = 2
F32, BF16 = jnp.float32, jnp.bfloat16


def scores_of(q, keys, slot):
    rows, depth = q.shape
    half, tokens = rows // 2, keys.shape[2]
    zero = jnp.zeros((half, depth), q.dtype)
    both = jnp.concatenate([jnp.concatenate([q[:half], zero], 1), jnp.concatenate([zero, q[half:]], 1)], 0)
    lane = lax.broadcasted_iota(jnp.int32, (tokens, rows), 1) % half
    scores = jnp.zeros((tokens, rows), F32)
    for pair in range(half):
        two = jnp.concatenate([keys[slot, pair], keys[slot, pair + half]], 1)
        got = lax.dot_general(two, both, (((1,), (1,)), ((), ())), preferred_element_type=F32)
        scores = jnp.where(lane == pair, got, scores)
    return scores


def seen_of(weights, values, slot, first):
    row = lax.broadcasted_iota(jnp.int32, (weights.shape[0], values.shape[3]), 0)
    out = jnp.zeros(row.shape, F32)
    for j in range(weights.shape[0]):
        out = jnp.where(row == j, jnp.dot(weights, values[slot, first + j], preferred_element_type=F32), out)
    return out


def kernel(n, inner, q_hbm, k_ref, v_ref, o_ref, q_ref, ring, scores, weights, stats, share, mine, parts_a, parts_b, last_mine, last_a, last_b, q_sem, ring_sem, recv_s, recv_a, recv_b, recv_la, recv_lb, sent):
    heads, rows, depth = q_ref.shape
    half, outer, piece = rows // 2, n // inner, rows // PIECES
    bulks, lasts = (heads - LAST) // BULK, LAST // TAIL
    first_last = bulks * BULK
    per = CHUNK // GROUP
    scale = depth**-0.5
    me = lax.axis_index("sp")
    core = lax.rem(me, 2)
    mine_a, mine_b = lax.rem(me, inner), me // inner * 2 + core
    base_a, base_b = me // inner * inner, lax.rem(me, inner) // 2 * 2
    def far_first(count):
        return sorted(range(1, count), key=lambda i: -min(i // 2 * 2, count - i // 2 * 2))

    peers_s = [lax.rem(me + i, n) for i in range(1, n)]
    peers_a = [(i, base_a + lax.rem(mine_a + i, inner)) for i in far_first(inner)]
    places_b = [lax.rem(mine_b + i, 2 * outer) for i in far_first(2 * outer)]
    peers_b = [place // 2 * inner + base_b + lax.rem(place, 2) for place in places_b]

    def fetch(ref, head, place):
        slot = lax.rem(place, SLOTS)
        return [
            pltpu.make_async_copy(ref.at[pl.ds(p * piece, piece), head], ring.at[slot, pl.ds(p * piece, piece)], ring_sem.at[slot, p])
            for p in range(PIECES)
        ]

    def fetch_k(head):
        return fetch(k_ref, head, head)

    def fetch_v(head):
        return fetch(v_ref, head, heads + head)

    def fetch_next(place, count):
        @pl.when(place < heads)
        def _():
            for g in range(count):
                for copy in fetch_k(place + g):
                    copy.start()

        @pl.when((place >= heads) & (place < 2 * heads))
        def _():
            for g in range(count):
                for copy in fetch_v(place + g - heads):
                    copy.start()

    def wait(copies):
        for copy in copies:
            copy.wait()

    fetch_q = pltpu.make_async_copy(q_hbm, q_ref, q_sem)
    fetch_q.start()
    for head in range(GROUP):
        for copy in fetch_k(head):
            copy.start()
    stats[...] = jnp.zeros(stats.shape, stats.dtype)

    barrier = pltpu.get_barrier_semaphore()
    for peer in peers_s:
        pl.semaphore_signal(barrier, inc=1, device_id={"sp": peer}, device_id_type=pl.DeviceIdType.MESH)
    for head in range(GROUP, SLOTS):
        for copy in fetch_k(head):
            copy.start()

    def send(source, target, peer, recv, place):
        pltpu.make_async_remote_copy(
            src_ref=source, dst_ref=target, send_sem=sent.at[place], recv_sem=recv, device_id={"sp": peer}, device_id_type=pl.DeviceIdType.MESH
        ).start()

    def arrived(ref, index, recv):
        some = ref.at[index, 0 : ref.shape[1] - 1]
        pltpu.make_async_copy(some, some, recv.at[index]).wait()

    def send_s(chunk):
        for peer in peers_s:
            send(stats.at[chunk, me], stats.at[chunk, me], peer, recv_s.at[chunk], 0)

    def send_a(own, parts, group, recv, place):
        for i, peer in peers_a:
            send(own.at[group, lax.rem(core + i, 2)], parts.at[group, mine_a], peer, recv.at[group], place)

    def send_b(parts, group, recv, place):
        for peer in peers_b:
            send(parts.at[group, mine_b], parts.at[group, mine_b], peer, recv.at[group], place)

    def weigh(group):
        for g in range(GROUP):
            head = group * GROUP + g
            scaled = scores[g] * scale
            high = jnp.max(scaled, 0, keepdims=True)
            w = jnp.exp(scaled - high)
            weights[head] = w.T.astype(BF16)
            chunk, j = head // CHUNK, lax.rem(head, CHUNK)
            stats[chunk, me, pl.ds(j, 1)] = jnp.concatenate([high, jnp.sum(w, 0, keepdims=True)], 1)

    def score(group):
        new = []
        for g in range(GROUP):
            head = group * GROUP + g
            new.append(scores_of(q_ref[head], ring, lax.rem(head, SLOTS)))
        for g in range(GROUP):
            scores[g] = new[g]

    def shares(chunk):
        top = stats[chunk, 0, :, :rows]
        for j in range(1, n):
            top = jnp.maximum(top, stats[chunk, j, :, :rows])
        total = jnp.zeros(top.shape, F32)
        for j in range(n):
            total = total + stats[chunk, j, :, rows:] * jnp.exp(stats[chunk, j, :, :rows] - top)
        columns = (jnp.exp(stats[chunk, me, :, :rows] - top) / total).T
        for j in range(CHUNK):
            share[chunk * CHUNK + j] = jnp.broadcast_to(columns[:, j : j + 1], (rows, depth))

    def part(own, group, g, head, h):
        at = slice(h * half, (h + 1) * half)
        seen = (seen_of(weights[head, at], ring, lax.rem(heads + head, SLOTS), h * half) * share[head, at]).astype(BF16)
        own[group, h, g] = seen
        return seen

    def keep(parts, group, g, seen):
        parts[group, mine_a, g] = jnp.where(core == 0, seen[0], seen[1])

    def block(parts, to, group, to_group, count):
        for g in range(count):
            out = parts[group, 0, g].astype(F32)
            for j in range(1, inner):
                out = out + parts[group, j, g].astype(F32)
            to[to_group, mine_b, g] = out.astype(BF16)

    def final(parts, group, head, count):
        for g in range(count):
            for h in range(2):
                out = parts[group, h, g].astype(F32)
                for j in range(1, outer):
                    out = out + parts[group, 2 * j + h, g].astype(F32)
                o_ref[head + g, h * half : (h + 1) * half] = out.astype(o_ref.dtype)

    fetch_q.wait()
    for g in range(GROUP):
        wait(fetch_k(g))
    score(0)
    fetch_next(SLOTS, GROUP)

    def keys_step(i, _):
        for g in range(GROUP):
            wait(fetch_k(i * GROUP + g))
        weigh(i - 1)
        score(i)
        fetch_next(i * GROUP + SLOTS, GROUP)

        @pl.when(i == per)
        def _():
            pl.semaphore_wait(barrier, n - 1)

        @pl.when(lax.rem(i, per) == 0)
        def _():
            send_s(i // per - 1)

        return 0

    lax.fori_loop(1, heads // GROUP, keys_step, 0)
    weigh(heads // GROUP - 1)
    send_s((heads - 1) // CHUNK)

    def ready_s(head):
        arrived(stats, head // CHUNK, recv_s)
        shares(head // CHUNK)

    def values_step(i, _):
        @pl.when(lax.rem(i, CHUNK // BULK) == 0)
        def _():
            ready_s(i * BULK)

        for g in range(BULK):
            wait(fetch_v(i * BULK + g))
        for g in range(BULK):
            keep(parts_a, i, g, [part(mine, i, g, i * BULK + g, h) for h in range(2)])
        send_a(mine, parts_a, i, recv_a, 1)
        fetch_next(heads + i * BULK + SLOTS, BULK)
        return 0

    lax.fori_loop(0, bulks, values_step, 0)

    def block_bulk(a):
        arrived(parts_a, a, recv_a)
        block(parts_a, parts_b, a, a, BULK)
        send_b(parts_b, a, recv_b, 2)

    def final_bulk(f):
        arrived(parts_b, f, recv_b)
        final(parts_b, f, f * BULK, BULK)

    def block_last(t):
        arrived(last_a, t, recv_la)
        block(last_a, last_b, t, t, TAIL)
        send_b(last_b, t, recv_lb, 4)

    def final_last(t):
        arrived(last_b, t, recv_lb)
        final(last_b, t, first_last + t * TAIL, TAIL)

    for t in range(lasts):
        for g in range(TAIL):
            head = first_last + t * TAIL + g
            if head % CHUNK == 0:
                ready_s(head)
            wait(fetch_v(head))
            keep(last_a, t, g, [part(last_mine, t, g, head, h) for h in range(2)])
        send_a(last_mine, last_a, t, recv_la, 3)
        if t < bulks - 1:
            block_bulk(t)
    for a in range(min(lasts, bulks - 1), bulks):
        block_bulk(a)
    for t in range(lasts):
        block_last(t)
    for f in range(bulks):
        final_bulk(f)
    for t in range(lasts):
        final_last(t)
    every = (stats.at[:, 0 : n - 1], parts_a.at[:, 0 : inner - 1], parts_b.at[:, 0 : 2 * outer - 1], last_a.at[:, 0 : inner - 1], last_b.at[:, 0 : 2 * outer - 1])
    for place, some in enumerate(every):
        pltpu.make_async_copy(some, some, sent.at[place]).wait()


def solution(mesh):
    n = mesh.shape["sp"]
    inner = 2 * math.isqrt(n // 2)
    outer = n // inner

    def step(q, k, v):
        q, k, v = q.transpose(1, 0, 2), k.transpose(0, 2, 1, 3), v.transpose(0, 2, 1, 3)
        heads, rows, depth = q.shape
        tokens, half = k.shape[2], rows // 2
        chunks, bulks, lasts = -(-heads // CHUNK), (heads - LAST) // BULK, LAST // TAIL
        whole = pl.BlockSpec(memory_space=pltpu.VMEM)
        out = pl.pallas_call(
            functools.partial(kernel, n, inner),
            out_shape=pltpu.VMEM(q.shape, q.dtype),
            in_specs=[pl.BlockSpec(memory_space=pl.ANY)] * 3,
            out_specs=whole,
            scratch_shapes=[
                pltpu.VMEM(q.shape, q.dtype),
                pltpu.VMEM((SLOTS, rows, tokens, depth), k.dtype),
                pltpu.VMEM((GROUP, tokens, rows), F32),
                pltpu.VMEM((heads, rows, tokens), BF16),
                pltpu.VMEM((chunks, n, CHUNK, 2 * rows), F32),
                pltpu.VMEM((chunks * CHUNK, rows, depth), F32),
                pltpu.VMEM((bulks, 2, BULK, half, depth), BF16),
                pltpu.VMEM((bulks, inner, BULK, half, depth), BF16),
                pltpu.VMEM((bulks, 2 * outer, BULK, half, depth), BF16),
                pltpu.VMEM((lasts, 2, TAIL, half, depth), BF16),
                pltpu.VMEM((lasts, inner, TAIL, half, depth), BF16),
                pltpu.VMEM((lasts, 2 * outer, TAIL, half, depth), BF16),
                pltpu.SemaphoreType.DMA,
                pltpu.SemaphoreType.DMA((SLOTS, PIECES)),
                pltpu.SemaphoreType.DMA((chunks,)),
                pltpu.SemaphoreType.DMA((bulks,)),
                pltpu.SemaphoreType.DMA((bulks,)),
                pltpu.SemaphoreType.DMA((lasts,)),
                pltpu.SemaphoreType.DMA((lasts,)),
                pltpu.SemaphoreType.DMA((5,)),
            ],
            compiler_params=pltpu.CompilerParams(collective_id=0, has_side_effects=True, vmem_limit_bytes=56 * 2**20),
            name="attend",
        )(q, k, v)
        return out.transpose(1, 0, 2)

    return jax.shard_map(
        step,
        mesh=mesh,
        in_specs=(P("dp", None, None), P("dp", "sp", None, None), P("dp", "sp", None, None)),
        out_specs=P("dp", None, None),
        check_vma=False,
    )
```
